256 devices in a mesh: lat: 16 (over z, y_hi), lon: 16 (over x, y_lo, core).
Axes of the slice: x: 4, y: 4 (y_hi: 2, y_lo: 2; y = y_hi * 2 + y_lo), z: 8, core: 2. Of those that a mesh axis runs over, the one named last changes fastest.
Arguments:
- x_fwd: bfloat16 [256, 1536, 256], P('lat', 'lon'), may hold values from -6 to 6
- x_prev: bfloat16 [256, 1536, 256], P('lat', 'lon'), may hold values from -6 to 6
- grad_out: bfloat16 [256, 1536, 256], P('lat', 'lon'), may hold values from -6 to 6
- weight: bfloat16 [2048, 256], replicated, may hold values from -0.125 to 0.125
- basis: bfloat16 [256, 8, 3, 49], P('lat'), may hold values from -1.5 to 1.5
- lon_reach: int32 [256], P('lat'), may hold values from 1 to 24, as said below
- lat_reach: int32 [256], P('lat'), may hold values from 0 to 1, as said below
Outputs:
- output: bfloat16 [256, 1536, 256], P('lat', 'lon')
- grad_in: bfloat16 [256, 1536, 256], P('lat', 'lon')
- grad_weight: float32 [2048, 256], P(('lat', 'lon'))
The draws below stay inside these ranges and needn't reach their ends.
Inputs may be any that keep to these rules, and one draw needn't show every extreme that they name: `lon_reach`: reaches widen toward the two poles; the cycles nearest the poles reach 24. `lat_reach`: the first and the last cycle of every aligned block of 16 cycles reach 1.
All inputs are finite; a program needn't handle non-finite values.
Results may differ from the reference program's by a relative error of at most 0.0049.
Values may be sent and summed in bfloat16 or wider, within the bound.
No kernel may reach another device: no remote copies, remote signals or barrier semaphores. Data moves between devices by JAX's collectives and lax.ppermute only.
A program may use at most 192 MiB of HBM per device.

```python
import jax
import jax.numpy as jnp
from jax import lax

C = 256
K = 8
ROWS_DEV = 16
REACH = 24
TAPS = 49
KC = 2048
NLAT = 256
NLON = 1536


def draw_lon_reach(key, part):
    cycle_ids = jnp.arange(NLAT, dtype=jnp.int32)
    pole_gap = jnp.minimum(cycle_ids, NLAT - 1 - cycle_ids)
    base_reach = 1 + REACH * 4 // (4 + pole_gap)
    jitter = jax.random.randint(jax.random.fold_in(key, 11), (NLAT,), 0, 3)
    return jnp.clip(base_reach + jitter - 1, 1, REACH).astype(jnp.int32)


def draw_lat_reach(key, part):
    cycle_ids = jnp.arange(NLAT, dtype=jnp.int32)
    place = cycle_ids % ROWS_DEV
    at_edge = (place == 0) | (place == ROWS_DEV - 1)
    random_reach = jax.random.randint(jax.random.fold_in(key, 23), (NLAT,), 0, 2)
    return jnp.where(at_edge, 1, random_reach).astype(jnp.int32)


def level_of(own_key, dims, cuts, smallest, top_value):
    def one(position, blocks):
        heights = jax.random.uniform(jax.random.fold_in(jax.random.fold_in(own_key, 6), position), (blocks,), jnp.float32, smallest / len(cuts), top_value / len(cuts))
        return jnp.repeat(jnp.exp(heights), dims[position] // blocks).reshape((-1,) + (1,) * (len(dims) - position - 1))

    level = one(*cuts[0])
    for cut in cuts[1:]:
        level = level * one(*cut)
    return level


def scatter_about(key, extent, width, reach, shards=(), kind=jnp.bfloat16):
    entries = width * jax.random.normal(key, extent, jnp.float32)
    if shards:
        entries = entries * level_of(key, extent, shards, -0.22, 0.18)
    return jnp.clip(entries, -reach, reach).astype(kind)


def setup_inputs(seed: int = 0) -> dict:
    seeds = jax.random.split(jax.random.key(seed), 8)
    return {
        "x_fwd": scatter_about(seeds[0], (NLAT, NLON, C), 1.0, 6.0, ((0, 16), (1, 16))),
        "x_prev": scatter_about(seeds[1], (NLAT, NLON, C), 1.0, 6.0, ((0, 16), (1, 16))),
        "grad_out": scatter_about(seeds[2], (NLAT, NLON, C), 1.0, 6.0, ((0, 16), (1, 16))),
        "weight": scatter_about(seeds[3], (KC, C), KC ** -0.5, 0.125),
        "basis": scatter_about(seeds[4], (NLAT, K, 3, TAPS), 0.25, 1.5, ((0, 16),)),
        "lon_reach": draw_lon_reach(jax.random.fold_in(seeds[7], 71), 0),
        "lat_reach": draw_lat_reach(jax.random.fold_in(seeds[7], 71), 0),
    }


def tap_filters(basis, lon_reach, lat_reach):
    lat_taps = jnp.arange(3, dtype=jnp.int32)
    lon_taps = jnp.arange(TAPS, dtype=jnp.int32)
    live_taps = (jnp.abs(lat_taps - 1)[None, :, None] <= lat_reach[:, None, None]) & (jnp.abs(lon_taps - REACH)[None, None, :] <= lon_reach[:, None, None])
    return jnp.where(live_taps[:, None, :, :], basis, jnp.zeros_like(basis))


def cycle_pad(source):
    cycle = jnp.concatenate([source[:, NLON - REACH:], source, source[:, :REACH]], axis=1)
    return jnp.pad(cycle, ((1, 1), (0, 0), (0, 0)))


def conv_row(padded, filter_row, row_id):
    window = lax.dynamic_slice_in_dim(padded, row_id, 3, 0).astype(jnp.float32)
    stacked = jnp.stack([window[:, shift_col:shift_col + NLON] for shift_col in range(TAPS)], axis=1)
    conv = jnp.einsum('kab,ablc->lkc', filter_row.astype(jnp.float32), stacked)
    return conv.reshape(NLON, KC).astype(jnp.bfloat16)


def spread_row(grad_conv, filter_row):
    grads = grad_conv.astype(jnp.float32).reshape(NLON, K, C)
    cycle = jnp.concatenate([grads[NLON - REACH:], grads, grads[:REACH]], axis=0)
    stacked = jnp.stack([cycle[2 * REACH - shift_col:2 * REACH - shift_col + NLON] for shift_col in range(TAPS)], axis=0)
    return jnp.einsum('kab,blkc->alc', filter_row.astype(jnp.float32), stacked)


def reference(x_fwd, x_prev, grad_out, weight, basis, lon_reach, lat_reach):
    filters = tap_filters(basis, lon_reach, lat_reach)
    pad_fwd = cycle_pad(x_fwd)
    pad_prev = cycle_pad(x_prev)
    row_ids = jnp.arange(NLAT, dtype=jnp.int32)

    def forward_row(row_id):
        filter_row = lax.dynamic_index_in_dim(filters, row_id, 0, keepdims=False)
        conv = conv_row(pad_fwd, filter_row, row_id)
        return jnp.dot(conv, weight, preferred_element_type=jnp.float32).astype(jnp.bfloat16)

    output = lax.map(forward_row, row_ids)

    def backward_row(carry, row_id):
        weight_sum, pending, pending_next = carry
        filter_row = lax.dynamic_index_in_dim(filters, row_id, 0, keepdims=False)
        conv = conv_row(pad_prev, filter_row, row_id)
        grad_row = lax.dynamic_index_in_dim(grad_out, row_id, 0, keepdims=False)
        weight_sum = weight_sum + lax.dot_general(conv, grad_row, (((0,), (0,)), ((), ())), preferred_element_type=jnp.float32)
        grad_conv = lax.dot_general(grad_row, weight, (((1,), (1,)), ((), ())), preferred_element_type=jnp.float32).astype(jnp.bfloat16)
        pieces = spread_row(grad_conv, filter_row)
        finished = pending + pieces[0]
        return (weight_sum, pending_next + pieces[1], pieces[2]), finished

    start_carry = (jnp.zeros((KC, C), jnp.float32), jnp.zeros((NLON, C), jnp.float32), jnp.zeros((NLON, C), jnp.float32))
    final_carry, finished = lax.scan(backward_row, start_carry, row_ids)
    grad_weight, pending, leftover = final_carry
    grad_in = jnp.concatenate([finished[1:], pending[None]], axis=0).astype(jnp.bfloat16)
    return output, grad_in, grad_weight
```

```python
import jax
import jax.numpy as jnp
from jax import lax
from jax.experimental import pallas as pl
from jax.experimental.pallas import tpu as pltpu
from jax.sharding import PartitionSpec as P


F32 = jnp.float32
BF16 = jnp.bfloat16
REACH = 24
GROUP = 32
SPAN = 80
LANES = 256
CONV_UNROLL = 16
GRAD_UNROLL = 8


def dot(lhs, rhs, dims):
    return lax.dot_general(lhs, rhs, (dims, ((), ())), preferred_element_type=F32)


def params():
    return pltpu.CompilerParams(vmem_limit_bytes=56 * 1024 * 1024)


def vmem(count):
    return [pl.BlockSpec(memory_space=pltpu.VMEM)] * count


def banded(taps):
    pieces = []
    for k in range(taps.shape[0]):
        wide = jnp.broadcast_to(taps[k : k + 1], (GROUP, LANES))
        pieces.append(pltpu.roll(wide, 0, 1, stride=1, stride_axis=0).astype(BF16))
    return jnp.concatenate(pieces, axis=0)


def grads_kernel(
    flat_ref, grad_ref, north_ref, south_ref, weight_ref, x_ref, bands_ref, core_ref, to_east_ref, to_west_ref, gc_ref, spread_ref
):
    rows, cols, chans = grad_ref.shape
    basis = flat_ref.shape[1]
    cells = rows * cols
    spread_ref[...] = jnp.zeros(spread_ref.shape, F32)
    grads = grad_ref[...].reshape(cells, chans)
    outer = jnp.concatenate([north_ref[2 * cols : 3 * cols, :], south_ref[2 * cols : 3 * cols, :]], axis=0)
    for k in range(basis):
        mix = weight_ref[k * chans : (k + 1) * chans, :]
        gc_ref[:cells, k * chans : (k + 1) * chans] = dot(grads, mix, (((1,), (1,)))).astype(BF16)
        gc_ref[cells:, k * chans : (k + 1) * chans] = dot(outer, mix, (((1,), (1,)))).astype(BF16)

    def spread_row(band, line, row, lat_taps):
        for g in range(cols // GROUP):
            first = line * cols + g * GROUP
            cell = jnp.concatenate(
                [gc_ref[pl.ds(first, GROUP), k * chans : (k + 1) * chans] for k in range(basis)], axis=0
            )
            part = dot(band, cell, (((0,), (0,))))
            for a in lat_taps:
                spread_ref[row + a, g * GROUP : g * GROUP + SPAN, :] += part[a * SPAN : (a + 1) * SPAN]

    def one_row(r, carry):
        band = banded(flat_ref[r].astype(F32))
        bands_ref[r] = band
        spread_row(band, r, r, range(3))
        return carry

    lax.fori_loop(0, rows, one_row, 0, unroll=GRAD_UNROLL)
    spread_row(banded(north_ref[3 * cols :, :].astype(F32)), rows, -1, (2,))
    spread_row(banded(south_ref[3 * cols :, :].astype(F32)), rows + 1, rows, (0,))
    core_ref[...] = spread_ref[1 : rows + 1, REACH : REACH + cols, :]
    tall = rows + 2
    for low, at, send_ref in ((0, 0, to_west_ref), (REACH + cols, cols - REACH, to_east_ref)):
        send_ref[tall:] = spread_ref[1 : rows + 1, low : low + REACH, :].astype(BF16)
        send_ref[1 : rows + 1] = x_ref[:, at : at + REACH, :]
        send_ref[0] = north_ref[cols + at : cols + at + REACH, :]
        send_ref[rows + 1] = south_ref[cols + at : cols + at + REACH, :]


def fill_padded(x_ref, north_ref, south_ref, place, west_ref, east_ref, padded_ref):
    rows, cols, chans = x_ref.shape
    padded_ref[:, 2 * REACH + cols - 16 :, :] = jnp.zeros((rows + 2, 32, chans), BF16)
    padded_ref[:, :REACH, :] = west_ref[: rows + 2]
    padded_ref[1 : rows + 1, REACH : REACH + cols, :] = x_ref[...]
    padded_ref[0, REACH : REACH + cols, :] = north_ref[place * cols : (place + 1) * cols, :]
    padded_ref[rows + 1, REACH : REACH + cols, :] = south_ref[place * cols : (place + 1) * cols, :]
    padded_ref[:, REACH + cols : 2 * REACH + cols, :] = east_ref[: rows + 2]


def convolve(bands_ref, padded_ref, conv_ref, rows, cols, chans):
    def one_row(r, carry):
        band = bands_ref[r]
        for g in range(cols // GROUP):
            low = g * GROUP
            window = jnp.concatenate(
                [
                    padded_ref[r, low : low + SPAN, :],
                    padded_ref[r + 1, low : low + SPAN, :],
                    padded_ref[r + 2, low : low + SPAN + 16, :],
                ],
                axis=0,
            )
            conv = dot(band, window, (((1,), (0,)))).astype(BF16)
            for k in range(band.shape[0] // GROUP):
                conv_ref[pl.ds(r * cols + low, GROUP), k * chans : (k + 1) * chans] = conv[
                    k * GROUP : (k + 1) * GROUP
                ]
        return carry

    lax.fori_loop(0, rows, one_row, 0, unroll=CONV_UNROLL)


def weight_kernel(
    core_ref, bands_ref, x_ref, north_ref, south_ref, west_ref, east_ref, grad_ref, keep_ref, send_ref, padded_ref, conv_ref
):
    rows, cols, chans = x_ref.shape
    fill_padded(x_ref, north_ref, south_ref, 0, west_ref, east_ref, padded_ref)
    convolve(bands_ref, padded_ref, conv_ref, rows, cols, chans)
    grads = grad_ref[...].reshape(rows * cols, chans)
    first = core_ref[0] == 0
    half = chans // 2
    for k in range(conv_ref.shape[1] // chans):
        part = dot(conv_ref[:, k * chans : (k + 1) * chans], grads, (((0,), (0,))))
        part = part.reshape(chans // 16, 2, 8, chans)
        even, odd = (part[:, 0].reshape(half, chans), part[:, 1].reshape(half, chans))
        keep_ref[k * half : (k + 1) * half, :] = jnp.where(first, even, odd)
        send_ref[k * half : (k + 1) * half, :] = jnp.where(first, odd, even).astype(BF16)


def forward_kernel(bands_ref, x_ref, north_ref, south_ref, west_ref, east_ref, weight_ref, out_ref, padded_ref, conv_ref):
    rows, cols, chans = x_ref.shape
    fill_padded(x_ref, north_ref, south_ref, 1, west_ref, east_ref, padded_ref)
    convolve(bands_ref, padded_ref, conv_ref, rows, cols, chans)
    step = 4
    for r in range(0, rows, step):
        out_ref[r : r + step] = (
            dot(conv_ref[r * cols : (r + step) * cols, :], weight_ref[...], (((1,), (0,))))
            .astype(BF16)
            .reshape(step, cols, chans)
        )


def finish_kernel(core_ref, west_ref, east_ref, out_ref):
    rows, cols, _ = out_ref.shape
    tall = rows + 2
    out_ref[:, REACH : cols - REACH, :] = core_ref[:, REACH : cols - REACH, :].astype(BF16)
    out_ref[:, :REACH, :] = (core_ref[:, :REACH, :] + west_ref[tall:].astype(F32)).astype(BF16)
    out_ref[:, cols - REACH :, :] = (core_ref[:, cols - REACH :, :] + east_ref[tall:].astype(F32)).astype(BF16)


def sent(value, axis, steps, periodic):
    count = lax.axis_size(axis)
    pairs = [(i, (i + steps) % count) for i in range(count) if periodic or 0 <= i + steps < count]
    return lax.ppermute(value, axis, pairs)


def bit_of(axis_bits):
    axis, bit = axis_bits
    return (lax.axis_index(axis) >> (bit.bit_length() - 1)) & 1


def exchanged(value, bits, flips):
    lat, lon = (lax.axis_size("lat"), lax.axis_size("lon"))
    lat_flip = sum(b for (axis, b), f in zip(bits, flips) if f and axis == "lat")
    lon_flip = sum(b for (axis, b), f in zip(bits, flips) if f and axis == "lon")
    pairs = []
    for i in range(lat):
        for j in range(lon):
            pairs.append((i * lon + j, (i ^ lat_flip) * lon + (j ^ lon_flip)))
    return lax.ppermute(value, ("lat", "lon"), pairs)


NAMES = (("lat", 8), ("lat", 4), ("lat", 2), ("lat", 1), ("lon", 8), ("lon", 4), ("lon", 2))


def stage(value, names, bits):
    dims = [names.index(b) for b in bits]
    own = [bit_of(b) for b in bits]

    def pick(flips):
        piece = value
        for dim, o, f in zip(dims, own, flips):
            piece = lax.dynamic_slice_in_dim(piece, o if not f else 1 - o, 1, dim)
        return jnp.squeeze(piece, tuple(dims))

    combos = [(1,)] if len(bits) == 1 else [(1, 1), (1, 0), (0, 1)]
    arrived = [exchanged(pick(flips).astype(BF16), bits, flips) for flips in combos]
    value = pick((0,) * len(bits))
    for piece in arrived:
        value = value + piece.astype(F32)
    return value, [n for n in names if n not in bits]


def scattered_sum(keep, send):
    names = list(NAMES)
    shape = (2,) * len(names) + (8, keep.shape[1])
    arrived = exchanged(send, (("lon", 1),), (1,))
    value = (keep + arrived.astype(F32)).reshape(shape)
    value, names = stage(value, names, (("lon", 2), ("lon", 4)))
    value, names = stage(value, names, (("lon", 8),))
    value = value.reshape((lax.axis_size("lat"),) + value.shape[-2:])
    return lax.all_to_all(value, "lat", 0, 0).sum(0)


def body(x_fwd, x_prev, grad_out, weight, basis, lon_reach, lat_reach):
    rows, cols, chans = x_fwd.shape
    basis_count = basis.shape[1]
    taps = basis.shape[3]
    cells = rows * cols
    wide = 2 * REACH + cols

    lane = jnp.arange(LANES, dtype=jnp.int32)
    live = (jnp.abs(lane // SPAN - 1)[None] <= lat_reach[:, None]) & (
        jnp.abs(lane % SPAN - REACH)[None] <= lon_reach[:, None]
    )
    flat = sum(
        jnp.pad(basis[:, :, a, :], ((0, 0), (0, 0), (a * SPAN, LANES - a * SPAN - taps))) for a in range(3)
    )
    flat = jnp.where(live[:, None, :], flat, jnp.zeros_like(flat))

    def line(r):
        return jnp.concatenate([x_prev[r], x_fwd[r], grad_out[r], flat[r]], axis=0)

    north = sent(line(rows - 1), "lat", 1, False)
    south = sent(line(0), "lat", -1, False)

    def tall_edge(field, low):
        edge = slice(low, low + REACH)
        return jnp.concatenate([north[None, edge], field[:, edge], south[None, edge]], axis=0)

    west_prev = sent(tall_edge(x_prev, cols - REACH), "lon", 1, True)
    east_prev = sent(tall_edge(x_prev, 0), "lon", -1, True)

    sides = jax.ShapeDtypeStruct((2 * rows + 2, REACH, chans), BF16)
    bands, core, to_east, to_west = pl.pallas_call(
        grads_kernel,
        out_shape=(
            jax.ShapeDtypeStruct((rows, basis_count * GROUP, LANES), BF16),
            jax.ShapeDtypeStruct((rows, cols, chans), F32),
            sides,
            sides,
        ),
        in_specs=vmem(6),
        out_specs=tuple(vmem(4)),
        scratch_shapes=[
            pltpu.VMEM((cells + 2 * cols, basis_count * chans), BF16),
            pltpu.VMEM((rows + 2, wide, chans), F32),
        ],
        compiler_params=params(),
        name="grads",
    )(flat, grad_out, north, south, weight, x_fwd)

    from_west = sent(to_east, "lon", 1, True)
    from_east = sent(to_west, "lon", -1, True)

    conv_scratch = [
        pltpu.VMEM((rows + 2, wide + 16, chans), BF16),
        pltpu.VMEM((cells, basis_count * chans), BF16),
    ]
    half = (weight.shape[0] // 2, chans)
    keep, send = pl.pallas_call(
        weight_kernel,
        out_shape=(jax.ShapeDtypeStruct(half, F32), jax.ShapeDtypeStruct(half, BF16)),
        in_specs=[pl.BlockSpec(memory_space=pltpu.SMEM)] + vmem(7),
        out_specs=tuple(vmem(2)),
        scratch_shapes=conv_scratch,
        compiler_params=params(),
        name="weight_grad",
    )(bit_of(("lon", 1)).reshape(1), bands, x_prev, north, south, west_prev, east_prev, grad_out)
    grad_weight = scattered_sum(keep, send)

    output = pl.pallas_call(
        forward_kernel,
        out_shape=jax.ShapeDtypeStruct(x_fwd.shape, BF16),
        in_specs=vmem(7),
        out_specs=vmem(1)[0],
        scratch_shapes=conv_scratch,
        compiler_params=params(),
        name="forward",
    )(bands, x_fwd, north, south, from_west, from_east, weight)

    grad_in = pl.pallas_call(
        finish_kernel,
        out_shape=jax.ShapeDtypeStruct(x_fwd.shape, BF16),
        in_specs=vmem(3),
        out_specs=vmem(1)[0],
        compiler_params=params(),
        name="finish",
    )(core, from_west, from_east)
    return (output, grad_in, grad_weight)


def solution(mesh):
    return jax.shard_map(
        body,
        mesh=mesh,
        in_specs=(
            P("lat", "lon", None),
            P("lat", "lon", None),
            P("lat", "lon", None),
            P(),
            P("lat", None, None, None),
            P("lat"),
            P("lat"),
        ),
        out_specs=(P("lat", "lon", None), P("lat", "lon", None), P(("lat", "lon"), None)),
        check_vma=False,
    )
```

```python
import jax
import jax.numpy as jnp
from jax import lax
from jax.experimental import pallas as pl
from jax.experimental.pallas import tpu as pltpu
from jax.sharding import PartitionSpec as P


F32 = jnp.float32
BF16 = jnp.bfloat16
REACH = 24
GROUP = 32
SPAN = 80
LANES = 256
CONV_UNROLL = 16
GRAD_UNROLL = 8


def dot(lhs, rhs, dims):
    return lax.dot_general(lhs, rhs, (dims, ((), ())), preferred_element_type=F32)


def params():
    return pltpu.CompilerParams(vmem_limit_bytes=24 * 1024 * 1024)


def vmem(count):
    return [pl.BlockSpec(memory_space=pltpu.VMEM)] * count


def banded(taps):
    pieces = []
    for k in range(taps.shape[0]):
        wide = jnp.broadcast_to(taps[k : k + 1], (GROUP, LANES))
        pieces.append(pltpu.roll(wide, 0, 1, stride=1, stride_axis=0).astype(BF16))
    return jnp.concatenate(pieces, axis=0)


def mix_kernel(flat_ref, grad_ref, weight_ref, bands_ref, gc_ref):
    rows, cols, chans = grad_ref.shape
    grads = grad_ref[...].reshape(rows * cols, chans)
    basis = flat_ref.shape[1]
    for k in range(basis):
        mix = weight_ref[k * chans : (k + 1) * chans, :]
        gc_ref[:, k * chans : (k + 1) * chans] = dot(grads, mix, (((1,), (1,)))).astype(BF16)
        for r in range(k * rows // basis, (k + 1) * rows // basis):
            bands_ref[r] = banded(flat_ref[r].astype(F32))


def grads_kernel(
    bands_ref, gc_ref, north_ref, south_ref, weight_ref, x_ref, core_ref, to_east_ref, to_west_ref, outer_ref, spread_ref
):
    rows, cols, chans = core_ref.shape
    basis = weight_ref.shape[0] // chans
    spread_ref[...] = jnp.zeros(spread_ref.shape, F32)
    outer = jnp.concatenate([north_ref[2 * cols : 3 * cols, :], south_ref[2 * cols : 3 * cols, :]], axis=0)
    for k in range(basis):
        mix = weight_ref[k * chans : (k + 1) * chans, :]
        outer_ref[:, k * chans : (k + 1) * chans] = dot(outer, mix, (((1,), (1,)))).astype(BF16)

    def spread_row(band, from_ref, line, row, lat_taps):
        for g in range(cols // GROUP):
            first = line * cols + g * GROUP
            cell = jnp.concatenate(
                [from_ref[pl.ds(first, GROUP), k * chans : (k + 1) * chans] for k in range(basis)], axis=0
            )
            part = dot(band, cell, (((0,), (0,))))
            for a in lat_taps:
                spread_ref[row + a, g * GROUP : g * GROUP + SPAN, :] += part[a * SPAN : (a + 1) * SPAN]

    def one_row(r, carry):
        spread_row(bands_ref[r], gc_ref, r, r, range(3))
        return carry

    lax.fori_loop(0, rows, one_row, 0, unroll=GRAD_UNROLL)
    spread_row(banded(north_ref[3 * cols :, :].astype(F32)), outer_ref, 0, -1, (2,))
    spread_row(banded(south_ref[3 * cols :, :].astype(F32)), outer_ref, 1, rows, (0,))
    core_ref[...] = spread_ref[1 : rows + 1, REACH : REACH + cols, :]
    tall = rows + 2
    for low, at, send_ref in ((0, 0, to_west_ref), (REACH + cols, cols - REACH, to_east_ref)):
        send_ref[tall:] = spread_ref[1 : rows + 1, low : low + REACH, :].astype(BF16)
        send_ref[1 : rows + 1] = x_ref[:, at : at + REACH, :]
        send_ref[0] = north_ref[cols + at : cols + at + REACH, :]
        send_ref[rows + 1] = south_ref[cols + at : cols + at + REACH, :]


def fill_padded(x_ref, north_ref, south_ref, place, west_ref, east_ref, padded_ref):
    rows, cols, chans = x_ref.shape
    padded_ref[:, 2 * REACH + cols - 16 :, :] = jnp.zeros((rows + 2, 32, chans), BF16)
    padded_ref[:, :REACH, :] = west_ref[: rows + 2]
    padded_ref[1 : rows + 1, REACH : REACH + cols, :] = x_ref[...]
    padded_ref[0, REACH : REACH + cols, :] = north_ref[place * cols : (place + 1) * cols, :]
    padded_ref[rows + 1, REACH : REACH + cols, :] = south_ref[place * cols : (place + 1) * cols, :]
    padded_ref[:, REACH + cols : 2 * REACH + cols, :] = east_ref[: rows + 2]


def convolve(bands_ref, padded_ref, conv_ref, rows, cols, chans):
    def one_row(r, carry):
        band = bands_ref[r]
        for g in range(cols // GROUP):
            low = g * GROUP
            window = jnp.concatenate(
                [
                    padded_ref[r, low : low + SPAN, :],
                    padded_ref[r + 1, low : low + SPAN, :],
                    padded_ref[r + 2, low : low + SPAN + 16, :],
                ],
                axis=0,
            )
            conv = dot(band, window, (((1,), (0,)))).astype(BF16)
            for k in range(band.shape[0] // GROUP):
                conv_ref[pl.ds(r * cols + low, GROUP), k * chans : (k + 1) * chans] = conv[
                    k * GROUP : (k + 1) * GROUP
                ]
        return carry

    lax.fori_loop(0, rows, one_row, 0, unroll=CONV_UNROLL)


def weight_kernel(
    core_ref, bands_ref, x_ref, north_ref, south_ref, west_ref, east_ref, grad_ref, keep_ref, send_ref, padded_ref, conv_ref
):
    rows, cols, chans = x_ref.shape
    fill_padded(x_ref, north_ref, south_ref, 0, west_ref, east_ref, padded_ref)
    convolve(bands_ref, padded_ref, conv_ref, rows, cols, chans)
    grads = grad_ref[...].reshape(rows * cols, chans)
    first = core_ref[0] == 0
    half = chans // 2
    for k in range(conv_ref.shape[1] // chans):
        part = dot(conv_ref[:, k * chans : (k + 1) * chans], grads, (((0,), (0,))))
        part = part.reshape(chans // 16, 2, 8, chans)
        even, odd = (part[:, 0].reshape(half, chans), part[:, 1].reshape(half, chans))
        keep_ref[k * half : (k + 1) * half, :] = jnp.where(first, even, odd)
        send_ref[k * half : (k + 1) * half, :] = jnp.where(first, odd, even).astype(BF16)


def forward_kernel(bands_ref, x_ref, north_ref, south_ref, west_ref, east_ref, weight_ref, out_ref, padded_ref, conv_ref):
    rows, cols, chans = x_ref.shape
    fill_padded(x_ref, north_ref, south_ref, 1, west_ref, east_ref, padded_ref)
    convolve(bands_ref, padded_ref, conv_ref, rows, cols, chans)
    step = 4
    for r in range(0, rows, step):
        out_ref[r : r + step] = (
            dot(conv_ref[r * cols : (r + step) * cols, :], weight_ref[...], (((1,), (0,))))
            .astype(BF16)
            .reshape(step, cols, chans)
        )


def finish_kernel(core_ref, west_ref, east_ref, out_ref):
    rows, cols, _ = out_ref.shape
    tall = rows + 2
    out_ref[:, REACH : cols - REACH, :] = core_ref[:, REACH : cols - REACH, :].astype(BF16)
    out_ref[:, :REACH, :] = (core_ref[:, :REACH, :] + west_ref[tall:].astype(F32)).astype(BF16)
    out_ref[:, cols - REACH :, :] = (core_ref[:, cols - REACH :, :] + east_ref[tall:].astype(F32)).astype(BF16)


def sent(value, axis, steps, periodic):
    count = lax.axis_size(axis)
    pairs = [(i, (i + steps) % count) for i in range(count) if periodic or 0 <= i + steps < count]
    return lax.ppermute(value, axis, pairs)


def bit_of(axis_bits):
    axis, bit = axis_bits
    return (lax.axis_index(axis) >> (bit.bit_length() - 1)) & 1


def exchanged(value, bits, flips):
    lat, lon = (lax.axis_size("lat"), lax.axis_size("lon"))
    lat_flip = sum(b for (axis, b), f in zip(bits, flips) if f and axis == "lat")
    lon_flip = sum(b for (axis, b), f in zip(bits, flips) if f and axis == "lon")
    pairs = []
    for i in range(lat):
        for j in range(lon):
            pairs.append((i * lon + j, (i ^ lat_flip) * lon + (j ^ lon_flip)))
    return lax.ppermute(value, ("lat", "lon"), pairs)


NAMES = (("lat", 8), ("lat", 4), ("lat", 2), ("lat", 1), ("lon", 8), ("lon", 4), ("lon", 2))


def stage(value, names, bits):
    dims = [names.index(b) for b in bits]
    own = [bit_of(b) for b in bits]

    def pick(flips):
        piece = value
        for dim, o, f in zip(dims, own, flips):
            piece = lax.dynamic_slice_in_dim(piece, o if not f else 1 - o, 1, dim)
        return jnp.squeeze(piece, tuple(dims))

    combos = [(1,)] if len(bits) == 1 else [(1, 1), (1, 0), (0, 1)]
    arrived = [exchanged(pick(flips).astype(BF16), bits, flips) for flips in combos]
    value = pick((0,) * len(bits))
    for piece in arrived:
        value = value + piece.astype(F32)
    return value, [n for n in names if n not in bits]


def scattered_sum(keep, send):
    names = list(NAMES)
    shape = (2,) * len(names) + (8, keep.shape[1])
    arrived = exchanged(send, (("lon", 1),), (1,))
    value = (keep + arrived.astype(F32)).reshape(shape)
    value, names = stage(value, names, (("lon", 2), ("lon", 4)))
    value, names = stage(value, names, (("lon", 8),))
    value = value.reshape((lax.axis_size("lat"),) + value.shape[-2:])
    return lax.all_to_all(value.astype(BF16), "lat", 0, 0).astype(F32).sum(0)


def body(x_fwd, x_prev, grad_out, weight, basis, lon_reach, lat_reach):
    rows, cols, chans = x_fwd.shape
    basis_count = basis.shape[1]
    taps = basis.shape[3]
    cells = rows * cols
    wide = 2 * REACH + cols

    lane = jnp.arange(LANES, dtype=jnp.int32)
    live = (jnp.abs(lane // SPAN - 1)[None] <= lat_reach[:, None]) & (
        jnp.abs(lane % SPAN - REACH)[None] <= lon_reach[:, None]
    )
    flat = sum(
        jnp.pad(basis[:, :, a, :], ((0, 0), (0, 0), (a * SPAN, LANES - a * SPAN - taps))) for a in range(3)
    )
    flat = jnp.where(live[:, None, :], flat, jnp.zeros_like(flat))

    def line(r):
        return jnp.concatenate([x_prev[r], x_fwd[r], grad_out[r], flat[r]], axis=0)

    north = sent(line(rows - 1), "lat", 1, False)
    south = sent(line(0), "lat", -1, False)

    def tall_edge(field, low):
        edge = slice(low, low + REACH)
        return jnp.concatenate([north[None, edge], field[:, edge], south[None, edge]], axis=0)

    west_prev = sent(tall_edge(x_prev, cols - REACH), "lon", 1, True)
    east_prev = sent(tall_edge(x_prev, 0), "lon", -1, True)

    bands, mixed = pl.pallas_call(
        mix_kernel,
        out_shape=(
            jax.ShapeDtypeStruct((rows, basis_count * GROUP, LANES), BF16),
            jax.ShapeDtypeStruct((cells, basis_count * chans), BF16),
        ),
        in_specs=vmem(3),
        out_specs=tuple(vmem(2)),
        compiler_params=params(),
        name="mix",
        cost_estimate=pl.CostEstimate(flops=3000000000, bytes_accessed=9000000, transcendentals=0),
    )(flat, grad_out, weight)

    sides = jax.ShapeDtypeStruct((2 * rows + 2, REACH, chans), BF16)
    core, to_east, to_west = pl.pallas_call(
        grads_kernel,
        out_shape=(jax.ShapeDtypeStruct((rows, cols, chans), F32), sides, sides),
        in_specs=vmem(6),
        out_specs=tuple(vmem(3)),
        scratch_shapes=[
            pltpu.VMEM((2 * cols, basis_count * chans), BF16),
            pltpu.VMEM((rows + 2, wide, chans), F32),
        ],
        compiler_params=params(),
        name="grads",
        cost_estimate=pl.CostEstimate(flops=4000000000, bytes_accessed=9000000, transcendentals=0),
    )(bands, mixed, north, south, weight, x_fwd)

    from_west = sent(to_east, "lon", 1, True)
    from_east = sent(to_west, "lon", -1, True)

    conv_scratch = [
        pltpu.VMEM((rows + 2, wide + 16, chans), BF16),
        pltpu.VMEM((cells, basis_count * chans), BF16),
    ]
    half = (weight.shape[0] // 2, chans)
    keep, send = pl.pallas_call(
        weight_kernel,
        out_shape=(jax.ShapeDtypeStruct(half, F32), jax.ShapeDtypeStruct(half, BF16)),
        in_specs=[pl.BlockSpec(memory_space=pltpu.SMEM)] + vmem(7),
        out_specs=tuple(vmem(2)),
        scratch_shapes=conv_scratch,
        compiler_params=params(),
        name="weight_grad",
        cost_estimate=pl.CostEstimate(flops=5000000000, bytes_accessed=6000000, transcendentals=0),
    )(bit_of(("lon", 1)).reshape(1), bands, x_prev, north, south, west_prev, east_prev, grad_out)
    grad_weight = scattered_sum(keep, send)

    output = pl.pallas_call(
        forward_kernel,
        out_shape=jax.ShapeDtypeStruct(x_fwd.shape, BF16),
        in_specs=vmem(7),
        out_specs=vmem(1)[0],
        scratch_shapes=conv_scratch,
        compiler_params=params(),
        name="forward",
        cost_estimate=pl.CostEstimate(flops=5000000000, bytes_accessed=6000000, transcendentals=0),
    )(bands, x_fwd, north, south, from_west, from_east, weight)

    grad_in = pl.pallas_call(
        finish_kernel,
        out_shape=jax.ShapeDtypeStruct(x_fwd.shape, BF16),
        in_specs=vmem(3),
        out_specs=vmem(1)[0],
        compiler_params=params(),
        name="finish",
        cost_estimate=pl.CostEstimate(flops=2000000000, bytes_accessed=6000000, transcendentals=0),
    )(core, from_west, from_east)
    return (output, grad_in, grad_weight)


def solution(mesh):
    return jax.shard_map(
        body,
        mesh=mesh,
        in_specs=(
            P("lat", "lon", None),
            P("lat", "lon", None),
            P("lat", "lon", None),
            P(),
            P("lat", None, None, None),
            P("lat"),
            P("lat"),
        ),
        out_specs=(P("lat", "lon", None), P("lat", "lon", None), P(("lat", "lon"), None)),
        check_vma=False,
    )
```
